256 devices in a mesh: replica: 2 (over z), expert: 64 (over y, x), sub: 2 (over core).
Axes of the slice: x: 8, y: 8, z: 2, core: 2. Of those that a mesh axis runs over, the one named last changes fastest.
The devices are a block of a 8x8x16 slice.
Arguments:
- tokens: bfloat16 [2048, 7168], P(('replica', 'expert', 'sub')), parts along dimension 0, may hold values from -6 to 6
- expert_ids: int32 [2048, 8], P(('replica', 'expert', 'sub')), parts along dimension 0, may hold values from 0 to 31, all different within a row; in each aligned block of 8 rows (0 to 7, 8 to 15, ...) at most 3 rows name the same one
- route_levels: int32 [2048, 8], P(('replica', 'expert', 'sub')), parts along dimension 0, may hold values from 1 to 255
- gate_proj: bfloat16 [64, 7168, 512], P('expert', None, 'sub'), may hold values from -0.0625 to 0.0625
- up_proj: bfloat16 [64, 7168, 512], P('expert', None, 'sub'), may hold values from -0.0625 to 0.0625
- down_proj: bfloat16 [64, 512, 7168], P('expert', 'sub'), may hold values from -0.1875 to 0.1875
Outputs:
- moe_out: bfloat16 [2048, 7168], P(('replica', 'expert', 'sub')), parts along dimension 0
The draws below stay inside these ranges and needn't reach their ends.
There are 2 independent parts, one for each index of `replica`. The reference program is written for one: setup_inputs(seed, part) draws one part's arguments, and reference() takes and returns one part's arrays. A program takes and returns all parts, laid end to end along the dimension named above; an argument that names none is the same for every part. Nothing has to cross between parts.
Inputs may be any that keep to these rules, and one draw needn't show every extreme that they name: `expert_ids`: each row names 8 different experts; among the 8 rows of one device no expert is named more than 3 times, and in some devices' rows one is named exactly 3 times.
All inputs are finite; a program needn't handle non-finite values.
Results may differ from the reference program's by a relative error of at most 0.013.
Values may be sent and summed in bfloat16 or wider, within the bound.
No kernel may reach another device: no remote copies, remote signals or barrier semaphores. Data moves between devices by JAX's collectives and lax.ppermute only.
A program may use at most 448 MiB of HBM per device.

```python
import math
import jax
import jax.numpy as jnp
import numpy as np
from jax import lax

D = 7168
FF = 1024
TOK_DEV = 8
EXPERTS = 32
TOPK = 8
CAP = 3
TOKENS = 1024
N_EXPERT = 64
N_SUB = 2


def set_ends(array, rng, least, top_value):
    shape = array.shape
    spot = [jax.random.randint(jax.random.fold_in(rng, axis), (), 0, shape[axis]) for axis in range(len(shape))]
    array = array.at[tuple(spot)].set(least)
    longest = shape.index(max(shape))
    spot[longest] = (spot[longest] + 1) % shape[longest]
    return array.at[tuple(spot)].set(top_value)


def block_levels(own_key, shape, cuts, smallest, largest):
    level, own = 1.0, jax.random.fold_in(own_key, 6)
    for dim, parts in cuts:
        draws = jnp.exp(jax.random.uniform(jax.random.fold_in(own, dim), (parts,), jnp.float32, smallest / len(cuts), largest / len(cuts)))
        level = level * jnp.repeat(draws, shape[dim] // parts).reshape([-1 if axis == dim else 1 for axis in range(len(shape))])
    return level


def deal_out(key, own, number, rows, amount, top, bound, lean):
    ranking = jax.random.permutation(key, amount)
    heavy_load, common = portions_of(amount, rows * top, bound, lean, True), portions_of(amount, rows * top, bound, lean, False)
    places = jnp.arange(amount)

    def named(lengths, offset_by):
        used = int((lengths > 0).sum())
        fixed = max(1, used // 4)
        passed = fixed + (places - fixed + offset_by * (used - fixed)) % max(1, amount - fixed)
        return jnp.zeros((amount,), jnp.int32).at[ranking[jnp.where(places < fixed, places, passed)]].set(jnp.asarray(lengths, jnp.int32))

    lengths = jnp.where(number % 4 == 0, named(heavy_load, number // 4), named(common, number - number // 4 - 1))
    mixed = jax.random.permutation(jax.random.fold_in(own, 3), amount)
    giver, taker = mixed[0:amount // 2 * 2:2], mixed[1:amount // 2 * 2:2]
    room = jnp.minimum(lengths[giver] - 1, bound - lengths[taker]) // 2
    room = jnp.where((giver == ranking[0]) | (taker == ranking[0]) | (lengths[taker] == 0), 0, jnp.maximum(room, 0))
    passed = jax.random.randint(jax.random.fold_in(own, 4), (amount // 2,), 0, 1 << 20) % (room + 1)
    lengths = lengths.at[giver].add(-passed).at[taker].add(passed)
    labels = jnp.searchsorted(jnp.cumsum(lengths), jnp.arange(rows * top), side="right").astype(jnp.int32)
    grid = labels.reshape(top, rows).T
    grid = grid[jax.random.permutation(jax.random.fold_in(own, 1), rows)]
    offset_by = jax.random.randint(jax.random.fold_in(own, 2), (rows, 1), 0, top)
    return jnp.take_along_axis(grid, (jnp.arange(top)[None, :] + offset_by) % top, axis=1)


def portions_of(count, total, bound, slope, full):
    portions = [(1 << 20) // math.isqrt(grade ** slope) + 1 for grade in range(1, count + 1)]
    largest = bound if full else min(bound, max(-(-total // count), total * portions[0] // sum(portions)))
    least = 1 if total - largest >= count - 1 else 0
    holding, surplus = [largest] + [least] * (count - 1), total - largest - least * (count - 1)
    while surplus > 0:
        free = [i for i in range(1, count) if holding[i] < largest] or [i for i in range(1, count) if holding[i] < bound]
        mass, budget = sum([portions[i] for i in free]), surplus
        for i in free:
            addition = min(bound - holding[i], max(1, budget * portions[i] // mass), surplus)
            holding[i] = holding[i] + addition
            surplus = surplus - addition
    return np.array(holding)


def noise(rng, dims, scale, most, split=(), held_as=jnp.bfloat16):
    drawn = jax.random.normal(rng, dims, jnp.float32) * scale
    if len(split) > 0:
        drawn = block_levels(rng, dims, split, -0.22, 0.18) * drawn
    return jnp.clip(drawn, min=-most, max=most).astype(held_as)


def setup_inputs(seed: int = 0, part: int = 0) -> dict:
    splits = jax.random.split(jax.random.key(seed), 7)
    own_keys = jax.random.split(jax.random.fold_in(splits[6], part), 7)
    tokens = noise(own_keys[0], (TOKENS, D), 1.0, 6.0, ((0, 128),))
    expert_ids_keys = jax.random.split(jax.random.fold_in(own_keys[1], 1), TOKENS // TOK_DEV)
    expert_ids_turns = jax.random.permutation(jax.random.fold_in(own_keys[1], 3), TOKENS // TOK_DEV)
    expert_ids = jax.vmap(lambda own, number: deal_out(jax.random.fold_in(own_keys[1], 2), own, number, TOK_DEV, EXPERTS, TOPK, CAP, 2))(expert_ids_keys, expert_ids_turns).reshape((TOKENS, TOPK))
    route_levels = set_ends(jax.random.randint(own_keys[2], (TOKENS, TOPK), 1, 256), jax.random.fold_in(own_keys[2], 1), 1, 255).astype(jnp.int32)
    gate_proj = noise(splits[3], (2 * EXPERTS, D, FF // 2), D ** -0.5, 0.0625, ((0, 64), (2, 2)))
    up_proj = noise(splits[4], (2 * EXPERTS, D, FF // 2), D ** -0.5, 0.0625, ((0, 64), (2, 2)))
    down_proj = noise(splits[5], (2 * EXPERTS, FF // 2, D), FF ** -0.5, 0.1875, ((0, 64), (1, 2)))
    return {"tokens": tokens, "expert_ids": expert_ids, "route_levels": route_levels, "gate_proj": gate_proj, "up_proj": up_proj, "down_proj": down_proj}


def reference(tokens, expert_ids, route_levels, gate_proj, up_proj, down_proj):
    devices = N_EXPERT * N_SUB
    quarter = FF // 4
    source = tokens.reshape(devices, TOK_DEV, D).astype(jnp.float32)
    picked = expert_ids.reshape(devices, TOK_DEV * TOPK)
    onehot = (picked[:, :, None] == jnp.arange(EXPERTS, dtype=jnp.int32)[None, None, :]).astype(jnp.int32)
    before = jnp.cumsum(onehot, axis=1, dtype=jnp.int32) - onehot
    slot_of = jnp.sum(before * onehot, axis=2)
    shares = route_levels.astype(jnp.float32)
    shares = shares / jnp.sum(shares, axis=1, keepdims=True)
    shares = shares.reshape(devices, TOK_DEV, TOPK)
    slot_range = jnp.arange(CAP, dtype=jnp.int32)

    def advance(running, expert):
        chosen = (picked == expert)[:, :, None] & (slot_of[:, :, None] == slot_range[None, None, :])
        placed = chosen.astype(jnp.float32).reshape(devices, TOK_DEV, TOPK, CAP)
        sender = jnp.sum(placed, axis=2)
        weighting = jnp.sum(placed * shares[:, :, :, None], axis=2)
        slot_rows = jnp.einsum("dtc,dtf->dcf", sender, source).astype(jnp.bfloat16).reshape(devices * CAP, D)
        index_low = (2 * expert).astype(jnp.int32)
        index_high = (2 * expert + 1).astype(jnp.int32)
        gate_full = jnp.concatenate([lax.dynamic_index_in_dim(gate_proj, index_low, 0, keepdims=False),
                                     lax.dynamic_index_in_dim(gate_proj, index_high, 0, keepdims=False)], axis=1)
        up_full = jnp.concatenate([lax.dynamic_index_in_dim(up_proj, index_low, 0, keepdims=False),
                                   lax.dynamic_index_in_dim(up_proj, index_high, 0, keepdims=False)], axis=1)
        down_full = jnp.concatenate([lax.dynamic_index_in_dim(down_proj, index_low, 0, keepdims=False),
                                     lax.dynamic_index_in_dim(down_proj, index_high, 0, keepdims=False)], axis=0)
        gate_vals = jnp.dot(slot_rows, gate_full, preferred_element_type=jnp.float32)
        up_vals = jnp.dot(slot_rows, up_full, preferred_element_type=jnp.float32)
        hidden = (jax.nn.silu(gate_vals) * up_vals).astype(jnp.bfloat16)
        summed = jnp.zeros((devices * CAP, D), jnp.float32)
        for portion in range(4):
            piece = jnp.dot(hidden[:, portion * quarter:(portion + 1) * quarter],
                            down_full[portion * quarter:(portion + 1) * quarter],
                            preferred_element_type=jnp.float32).astype(jnp.bfloat16)
            piece = lax.optimization_barrier(piece)
            summed = summed + piece.astype(jnp.float32)
        rounded = lax.optimization_barrier(summed.astype(jnp.bfloat16))
        expert_out = rounded.astype(jnp.float32).reshape(devices, CAP, D)
        running = running + jnp.einsum("dtc,dcf->dtf", weighting, expert_out, precision=lax.Precision.HIGHEST)
        return running, None

    start = jnp.zeros((devices, TOK_DEV, D), jnp.float32)
    running, _ = lax.scan(advance, start, jnp.arange(EXPERTS, dtype=jnp.int32))
    return running.reshape(devices * TOK_DEV, D).astype(jnp.bfloat16)
```

```python
import math

import jax
import jax.numpy as jnp
from jax import lax
from jax.experimental import pallas as pl
from jax.experimental.pallas import tpu as pltpu
from jax.sharding import PartitionSpec as P

GROUP = ("expert", "sub")
INFO = 128
CAP = 3


def crossing_groups(side):
    def at(y, x, c):
        return (y * side + x) * 2 + c

    r = range(side)
    along_y = [[[at(y, x, c) for y in r] for x in r] for c in (0, 1)]
    along_x = [[[at(y, x, c) for x in r] for y in r] for c in (0, 1)]
    return along_y[0] + along_x[1], along_x[0] + along_y[1]


def route_kernel(experts_ref, rows_ref, send_ref, mix_ref, *, side, picks, width):
    toks = rows_ref.shape[0]
    info = rows_ref[:, width:].astype(jnp.float32)
    info = jnp.concatenate([info, jnp.zeros((INFO - toks, INFO), jnp.float32)], axis=0)
    info = info.T
    ids = info[:picks]
    levels = info[picks : 2 * picks]
    total = jnp.sum(levels, axis=0, keepdims=True)
    total = jnp.where(total == 0.0, 1.0, total)
    named, share = [], []
    for i in range(side):
        hit = ids == experts_ref[i].astype(jnp.float32)
        named.append(jnp.sum(jnp.where(hit, 1.0, 0.0), axis=0, keepdims=True))
        share.append(jnp.sum(jnp.where(hit, levels, 0.0), axis=0, keepdims=True) / total)
    named_all = jnp.concatenate(named, axis=0)
    per = toks // side
    a = lax.broadcasted_iota(jnp.int32, (INFO, INFO), 0)
    b = lax.broadcasted_iota(jnp.int32, (INFO, INFO), 1)
    earlier = jnp.where((a // per == b // per) & (a < b), 1.0, 0.0).astype(jnp.bfloat16)
    slot = jnp.dot(named_all.astype(jnp.bfloat16), earlier, preferred_element_type=jnp.float32)
    own = (
        lax.broadcasted_iota(jnp.int32, (side, INFO), 1) // per
        == lax.broadcasted_iota(jnp.int32, (side, INFO), 0)
    )
    pieces, mixes = [], []
    for i in range(side):
        for s in range(CAP):
            here = jnp.where(slot[i : i + 1] == float(s), named[i], 0.0)
            pieces.append(jnp.where(own, here, 0.0))
            mixes.append(jnp.where(own, here * share[i], 0.0))
    select = jnp.concatenate(pieces, axis=0)[:, :toks].astype(jnp.bfloat16)
    count = select.shape[0]
    mix = jnp.concatenate(mixes, axis=0)
    pad = -count % INFO
    mix = jnp.concatenate([mix, jnp.zeros((pad, INFO), jnp.float32)], axis=0).T
    mix = mix[:toks, :count]
    high = mix.astype(jnp.bfloat16)
    rest = mix - high.astype(jnp.float32)
    mid = rest.astype(jnp.bfloat16)
    low = (rest - mid.astype(jnp.float32)).astype(jnp.bfloat16)
    mix_ref[0:toks] = high
    mix_ref[toks : 2 * toks] = mid
    mix_ref[2 * toks : 3 * toks] = low
    step = 1024
    for n in range(width // step):
        cols = slice(n * step, (n + 1) * step)
        send_ref[:, cols] = jnp.dot(
            select, rows_ref[:, cols], preferred_element_type=jnp.float32
        ).astype(jnp.bfloat16)


def hidden_kernel(x_ref, ga_ref, gb_ref, ua_ref, ub_ref, out_ref, acc_ref):
    k = pl.program_id(0)
    part = ga_ref.shape[1]

    @pl.when(k == 0)
    def _():
        acc_ref[...] = jnp.zeros_like(acc_ref)

    x = x_ref[...]
    for n, w in enumerate((ga_ref, gb_ref, ua_ref, ub_ref)):
        acc_ref[:, n * part : (n + 1) * part] += jnp.dot(
            x, w[...], preferred_element_type=jnp.float32
        )

    @pl.when(k == pl.num_programs(0) - 1)
    def _():
        gate = acc_ref[:, : 2 * part]
        up = acc_ref[:, 2 * part :]
        out_ref[...] = (gate / (1.0 + jnp.exp(-gate)) * up).astype(jnp.bfloat16)


def down_kernel(h_ref, da_ref, db_ref, out_ref):
    part = da_ref.shape[0]
    out_ref[...] = (
        jnp.dot(h_ref[:, :part], da_ref[...], preferred_element_type=jnp.float32)
        + jnp.dot(h_ref[:, part:], db_ref[...], preferred_element_type=jnp.float32)
    ).astype(jnp.bfloat16)


def mix_kernel(mix_ref, rows_ref, out_ref):
    toks = out_ref.shape[0]
    y = jnp.dot(mix_ref[...], rows_ref[...], preferred_element_type=jnp.float32)
    out_ref[...] = (y[:toks] + y[toks : 2 * toks] + y[2 * toks :]).astype(jnp.bfloat16)


def local(tokens, expert_ids, route_levels, gate_proj, up_proj, down_proj):
    mine, width = tokens.shape
    picks = expert_ids.shape[1]
    chips = lax.axis_size("expert")
    side = math.isqrt(chips)
    first, second = crossing_groups(side)
    core = lax.axis_index("sub")
    chip = lax.axis_index("expert")
    y, x = chip // side, chip % side
    i = jnp.arange(side, dtype=jnp.int32)
    experts = jnp.where(core == 0, (y * side + i) // 2, (i * side + x) // 2)

    swap = [(0, 1), (1, 0)]
    gate_peer, up_peer, down_peer = (
        lax.ppermute(w, "sub", swap) for w in (gate_proj, up_proj, down_proj)
    )

    info = jnp.concatenate(
        [expert_ids, route_levels, jnp.zeros((mine, INFO - 2 * picks), jnp.int32)], axis=1
    )
    rows = jnp.concatenate([tokens, info.astype(jnp.bfloat16)], axis=1)
    rows = lax.all_gather(rows, GROUP, axis=0, tiled=True, axis_index_groups=first)

    toks = side * mine
    slots = toks * CAP
    send, mix = pl.pallas_call(
        lambda *refs: route_kernel(*refs, side=side, picks=picks, width=width),
        out_shape=(
            jax.ShapeDtypeStruct((slots, width), jnp.bfloat16),
            jax.ShapeDtypeStruct((3 * toks, slots), jnp.bfloat16),
        ),
        in_specs=[
            pl.BlockSpec(memory_space=pltpu.SMEM),
            pl.BlockSpec(memory_space=pltpu.VMEM),
        ],
        out_specs=(
            pl.BlockSpec(memory_space=pltpu.VMEM),
            pl.BlockSpec(memory_space=pltpu.VMEM),
        ),
        name="route",
    )(experts, rows)

    def crossed(block):
        block = block.reshape(side, -1, width)
        block = lax.all_to_all(block, GROUP, 0, 0, tiled=True, axis_index_groups=second)
        return block.reshape(-1, width)

    arrived = crossed(send)

    part = gate_proj.shape[2]
    kb = 1024
    weight = pl.BlockSpec((None, kb, part), lambda k: (0, k, 0))
    hidden = pl.pallas_call(
        hidden_kernel,
        grid=(width // kb,),
        in_specs=[pl.BlockSpec((slots, kb), lambda k: (0, k)), weight, weight, weight, weight],
        out_specs=pl.BlockSpec((slots, 2 * part), lambda k: (0, 0)),
        out_shape=jax.ShapeDtypeStruct((slots, 2 * part), jnp.bfloat16),
        scratch_shapes=[pltpu.VMEM((slots, 4 * part), jnp.float32)],
        name="hidden",
    )(arrived, gate_proj, gate_peer, up_proj, up_peer)

    nb = 1024
    down = pl.BlockSpec((None, part, nb), lambda n: (0, 0, n))
    terms = pl.pallas_call(
        down_kernel,
        grid=(width // nb,),
        in_specs=[pl.BlockSpec((slots, 2 * part), lambda n: (0, 0)), down, down],
        out_specs=pl.BlockSpec((slots, nb), lambda n: (0, n)),
        out_shape=jax.ShapeDtypeStruct((slots, width), jnp.bfloat16),
        name="down",
    )(hidden, down_proj, down_peer)

    returned = crossed(terms)

    mixed = pl.pallas_call(
        mix_kernel,
        grid=(width // nb,),
        in_specs=[
            pl.BlockSpec((3 * toks, slots), lambda n: (0, 0)),
            pl.BlockSpec((slots, nb), lambda n: (0, n)),
        ],
        out_specs=pl.BlockSpec((toks, nb), lambda n: (0, n)),
        out_shape=jax.ShapeDtypeStruct((toks, width), jnp.bfloat16),
        name="mix",
    )(mix, returned)

    sums = lax.all_to_all(
        mixed.reshape(side, mine, width), GROUP, 0, 0, tiled=True, axis_index_groups=first
    )
    return jnp.sum(sums.astype(jnp.float32), axis=0).astype(jnp.bfloat16)


def solution(mesh):
    return jax.shard_map(
        local,
        mesh=mesh,
        in_specs=(
            P(("replica", "expert", "sub"), None),
            P(("replica", "expert", "sub"), None),
            P(("replica", "expert", "sub"), None),
            P("expert", None, "sub"),
            P("expert", None, "sub"),
            P("expert", "sub", None),
        ),
        out_specs=P(("replica", "expert", "sub"), None),
        check_vma=False,
    )
```

```python
import functools
import math

import jax
import jax.numpy as jnp
from jax import lax
from jax.experimental import pallas as pl
from jax.experimental.pallas import tpu as pltpu
from jax.sharding import PartitionSpec as P

GROUP = ("expert", "sub")
LANES = 128
INFO = 2 * LANES
CAP = 3
CHUNKS = 2


def shifts(side, k):
    first, second = [], []
    for y in range(side):
        for x in range(side):
            for c in (0, 1):
                here = (y * side + x) * 2 + c
                down = (((y + k) % side) * side + x) * 2 + c
                over = (y * side + (x + k) % side) * 2 + c
                first.append((here, down if c == 0 else over))
                second.append((here, over if c == 0 else down))
    return first, second


def moved(block, side, k, stage):
    return lax.ppermute(block, GROUP, shifts(side, k)[stage]) if k % side else block


def whole(shape=None):
    return pl.BlockSpec(memory_space=pltpu.VMEM)


def stacked(refs, cols=slice(None)):
    return jnp.concatenate([r[:, cols].astype(jnp.float32) for r in refs], axis=0)


def pack_kernel(tokens_ref, ids_ref, levels_ref, *outs):
    size = outs[-1].shape[1]
    picks = ids_ref.shape[1]
    for c, out in enumerate(outs):
        out[:, :size] = tokens_ref[:, c * size : (c + 1) * size]
    first = outs[0]
    first[:, size:] = jnp.zeros((first.shape[0], INFO), jnp.bfloat16)
    first[:, size : size + picks] = ids_ref[...].astype(jnp.float32).astype(jnp.bfloat16)
    first[:, size + LANES : size + LANES + picks] = (
        levels_ref[...].astype(jnp.float32).astype(jnp.bfloat16)
    )


def selection(experts_ref, info, side, picks, toks):
    info = jnp.concatenate([info, jnp.zeros((LANES - toks, INFO), jnp.float32)], axis=0)
    ids = info[:, :LANES].T[:picks]
    levels = info[:, LANES:].T[:picks]
    total = jnp.sum(levels, axis=0, keepdims=True)
    total = jnp.where(total == 0.0, 1.0, total)
    named, share = [], []
    for i in range(side):
        hit = ids == experts_ref[i].astype(jnp.float32)
        named.append(jnp.sum(jnp.where(hit, 1.0, 0.0), axis=0, keepdims=True))
        share.append(jnp.sum(jnp.where(hit, levels, 0.0), axis=0, keepdims=True) / total)
    per = toks // side
    a = lax.broadcasted_iota(jnp.int32, (LANES, LANES), 0)
    b = lax.broadcasted_iota(jnp.int32, (LANES, LANES), 1)
    earlier = jnp.where((a // per == b // per) & (a < b), 1.0, 0.0).astype(jnp.bfloat16)
    slot = jnp.dot(
        jnp.concatenate(named, axis=0).astype(jnp.bfloat16),
        earlier,
        preferred_element_type=jnp.float32,
    )
    own = (
        lax.broadcasted_iota(jnp.int32, (side, LANES), 1) // per
        == lax.broadcasted_iota(jnp.int32, (side, LANES), 0)
    )
    pieces, mixes = [], []
    for i in range(side):
        for s in range(CAP):
            here = jnp.where(slot[i : i + 1] == float(s), named[i], 0.0)
            pieces.append(jnp.where(own, here, 0.0))
            mixes.append(jnp.where(own, here * share[i], 0.0))
    select = jnp.concatenate(pieces, axis=0)[:, :toks].astype(jnp.bfloat16)
    count = select.shape[0]
    mix = jnp.concatenate(mixes + [jnp.zeros((-count % LANES, LANES), jnp.float32)], axis=0).T
    mix = mix[:toks, :count]
    high = mix.astype(jnp.bfloat16)
    rest = mix - high.astype(jnp.float32)
    mid = rest.astype(jnp.bfloat16)
    low = (rest - mid.astype(jnp.float32)).astype(jnp.bfloat16)
    return select, (high, mid, low)


def spread(select, rows, outs, size):
    step = 4 * LANES
    each = outs[0].shape[0]
    for n in range(size // step):
        cols = slice(n * step, (n + 1) * step)
        block = stacked(rows, cols).astype(jnp.bfloat16)
        got = jnp.dot(select, block, preferred_element_type=jnp.float32)
        for k, out in enumerate(outs):
            out[:, cols] = got[k * each : (k + 1) * each].astype(jnp.bfloat16)


def route_kernel(*refs, side, picks, size):
    experts_ref, rows = refs[0], refs[1 : 1 + side]
    select_ref, mix_ref, outs = refs[1 + side], refs[2 + side], refs[3 + side :]
    toks = select_ref.shape[1]
    select, mix = selection(experts_ref, stacked(rows, slice(size, size + INFO)), side, picks, toks)
    select_ref[...] = select
    for n, m in enumerate(mix):
        mix_ref[n * toks : (n + 1) * toks] = m
    spread(select, rows, outs, size)


def spread_kernel(*refs, side, size):
    spread(refs[0][...], refs[1 : 1 + side], refs[1 + side :], size)


def hidden_kernel(*refs, side, last):
    rows, weights = refs[:side], refs[side : side + 4]
    k = pl.program_id(0)
    part = weights[0].shape[1]
    acc = refs[-1]
    if last:
        start, out = refs[side + 4], refs[side + 5]

        @pl.when(k == 0)
        def _():
            acc[...] = start[...]
    else:

        @pl.when(k == 0)
        def _():
            acc[...] = jnp.zeros_like(acc)

    x = stacked(rows).astype(jnp.bfloat16)
    for n, w in enumerate(weights):
        acc[:, n * part : (n + 1) * part] += jnp.dot(x, w[...], preferred_element_type=jnp.float32)

    if last:

        @pl.when(k == pl.num_programs(0) - 1)
        def _():
            gate = acc[:, : 2 * part]
            up = acc[:, 2 * part :]
            out[...] = (gate / (1.0 + jnp.exp(-gate)) * up).astype(jnp.bfloat16)


def down_kernel(h_ref, da_ref, db_ref, *outs):
    part = da_ref.shape[0]
    y = jnp.dot(h_ref[:, :part], da_ref[...], preferred_element_type=jnp.float32) + jnp.dot(
        h_ref[:, part:], db_ref[...], preferred_element_type=jnp.float32
    )
    each = outs[0].shape[0]
    for k, out in enumerate(outs):
        out[...] = y[k * each : (k + 1) * each].astype(jnp.bfloat16)


def mix_kernel(mix_ref, *refs, side):
    rows, outs = refs[:side], refs[side:]
    each = outs[0].shape[0]
    toks = each * side
    y = jnp.dot(
        mix_ref[...], stacked(rows).astype(jnp.bfloat16), preferred_element_type=jnp.float32
    )
    y = y[:toks] + y[toks : 2 * toks] + y[2 * toks :]
    for k, out in enumerate(outs):
        out[...] = y[k * each : (k + 1) * each].astype(jnp.bfloat16)


def sum_kernel(*refs, side):
    out = refs[-1]
    size = refs[0].shape[1]
    for c in range(out.shape[1] // size):
        total = refs[c * side][...].astype(jnp.float32)
        for r in refs[c * side + 1 : (c + 1) * side]:
            total = total + r[...].astype(jnp.float32)
        out[:, c * size : (c + 1) * size] = total.astype(jnp.bfloat16)


def local(tokens, expert_ids, route_levels, gate_proj, up_proj, down_proj):
    mine, width = tokens.shape
    picks = expert_ids.shape[1]
    side = math.isqrt(lax.axis_size("expert"))
    core = lax.axis_index("sub")
    chip = lax.axis_index("expert")
    y, x = chip // side, chip % side
    k = jnp.arange(side, dtype=jnp.int32)
    experts = jnp.where(
        core == 0, (y * side + (x + k) % side) // 2, ((y + k) % side * side + x) // 2
    )
    size = width // CHUNKS
    toks = side * mine
    each = mine * CAP
    slots = side * each
    part = gate_proj.shape[2]

    def shape(*dims, dtype=jnp.bfloat16):
        return jax.ShapeDtypeStruct(dims, dtype)

    packed = pl.pallas_call(
        pack_kernel,
        out_shape=[shape(mine, size + (INFO if c == 0 else 0)) for c in range(CHUNKS)],
        name="pack",
    )(tokens, expert_ids, route_levels)

    gathered = [[moved(rows, side, k, 0) for k in range(side)] for rows in packed]

    swap = [(0, 1), (1, 0)]
    gate_peer, up_peer, down_peer = (
        lax.ppermute(w, "sub", swap) for w in (gate_proj, up_proj, down_proj)
    )

    arrived = []
    for c in range(CHUNKS):
        outs = [shape(each, size) for _ in range(side)]
        if c == 0:
            select, mix, *sent = pl.pallas_call(
                functools.partial(route_kernel, side=side, picks=picks, size=size),
                out_shape=[shape(slots, toks), shape(3 * toks, slots)] + outs,
                in_specs=[pl.BlockSpec(memory_space=pltpu.SMEM)] + [whole()] * side,
                name="route",
            )(experts, *gathered[c])
        else:
            sent = pl.pallas_call(
                functools.partial(spread_kernel, side=side, size=size),
                out_shape=outs,
                name="spread",
            )(select, *gathered[c])
        arrived.append([moved(b, side, k, 1) for k, b in enumerate(sent)])

    kb = 7 * LANES
    steps = size // kb
    acc = None
    for c in range(CHUNKS):
        last = c == CHUNKS - 1
        weight = pl.BlockSpec((None, kb, part), lambda k, c=c: (0, c * steps + k, 0))
        full = pl.BlockSpec((slots, 4 * part), lambda k: (0, 0))
        half = pl.BlockSpec((slots, 2 * part), lambda k: (0, 0))
        ops = [*arrived[c], gate_proj, gate_peer, up_proj, up_peer]
        specs = [pl.BlockSpec((each, kb), lambda k: (0, k))] * side + [weight] * 4
        if c:
            ops.append(acc)
            specs.append(full)
        acc = pl.pallas_call(
            functools.partial(hidden_kernel, side=side, last=last),
            grid=(steps,),
            in_specs=specs,
            out_specs=half if last else full,
            out_shape=shape(slots, 2 * part) if last else shape(slots, 4 * part, dtype=jnp.float32),
            scratch_shapes=[pltpu.VMEM((slots, 4 * part), jnp.float32)] if last else [],
            name="hidden",
        )(*ops)
    hidden = acc

    returned = []
    for c in range(CHUNKS):
        down = pl.BlockSpec((None, part, kb), lambda n, c=c: (0, 0, c * steps + n))
        terms = pl.pallas_call(
            down_kernel,
            grid=(steps,),
            in_specs=[pl.BlockSpec((slots, 2 * part), lambda n: (0, 0)), down, down],
            out_specs=[pl.BlockSpec((each, kb), lambda n: (0, n))] * side,
            out_shape=[shape(each, size) for _ in range(side)],
            name="down",
        )(hidden, down_proj, down_peer)
        returned.append([moved(b, side, -k, 1) for k, b in enumerate(terms)])

    parts = []
    for c in range(CHUNKS):
        mixed = pl.pallas_call(
            functools.partial(mix_kernel, side=side),
            grid=(steps,),
            in_specs=[pl.BlockSpec((3 * toks, slots), lambda n: (0, 0))]
            + [pl.BlockSpec((each, kb), lambda n: (0, n))] * side,
            out_specs=[pl.BlockSpec((mine, kb), lambda n: (0, n))] * side,
            out_shape=[shape(mine, size) for _ in range(side)],
            name="mix",
        )(mix, *returned[c])
        parts += [moved(b, side, -k, 0) for k, b in enumerate(mixed)]

    return pl.pallas_call(
        functools.partial(sum_kernel, side=side),
        out_shape=shape(mine, width),
        name="sum",
    )(*parts)


def solution(mesh):
    return jax.shard_map(
        local,
        mesh=mesh,
        in_specs=(
            P(("replica", "expert", "sub"), None),
            P(("replica", "expert", "sub"), None),
            P(("replica", "expert", "sub"), None),
            P("expert", None, "sub"),
            P("expert", None, "sub"),
            P("expert", "sub", None),
        ),
        out_specs=P(("replica", "expert", "sub"), None),
        check_vma=False,
    )
```

```python
import functools
import math

import jax
import jax.numpy as jnp
from jax import lax
from jax.experimental import pallas as pl
from jax.experimental.pallas import tpu as pltpu
from jax.sharding import PartitionSpec as P


GROUP = ("expert", "sub")
LANES = 128
INFO = 2 * LANES
CAP = 3
STEPS = 4
MIB = 1 << 20


def crossing_groups(side):
    def at(y, x, c):
        return (y * side + x) * 2 + c

    r = range(side)
    along_y = [[[at(y, x, c) for y in r] for x in r] for c in (0, 1)]
    along_x = [[[at(y, x, c) for x in r] for y in r] for c in (0, 1)]
    return along_y[0] + along_x[1], along_x[0] + along_y[1]


def held_in(x, space):
    return pltpu.with_memory_space_constraint(x, space)


V = pltpu.VMEM
S = pltpu.SMEM
A = pltpu.HBM
PLAIN = None


def call(kernel, ins, outs, scratch=(), limit=16):
    got = pl.pallas_call(
        kernel,
        in_specs=[pl.BlockSpec(memory_space=V if space is PLAIN else space) for _, space in ins],
        out_shape=[
            V(shape, dtype) if space is V else jax.ShapeDtypeStruct(shape, dtype)
            for shape, dtype, space in outs
        ],
        out_specs=[pl.BlockSpec(memory_space=V) for _ in outs],
        scratch_shapes=list(scratch),
        compiler_params=pltpu.CompilerParams(vmem_limit_bytes=limit * MIB),
    )(*[x if space is S else held_in(x, A if space is PLAIN else space) for x, space in ins])
    return got[0] if len(outs) == 1 else got


def pack_kernel(tokens_ref, ids_ref, levels_ref, out):
    mine, width = tokens_ref.shape
    picks = ids_ref.shape[1]
    rest = jnp.zeros((mine, LANES - picks), jnp.float32)
    info = [
        jnp.concatenate([r[...].astype(jnp.float32), rest], axis=1).astype(jnp.bfloat16)
        for r in (ids_ref, levels_ref)
    ]
    for i in range(out.shape[0] // mine):
        here = slice(i * mine, (i + 1) * mine)
        out[here, :width] = tokens_ref[...]
        out[here, width : width + LANES] = info[0]
        out[here, width + LANES :] = info[1]


def selection(experts_ref, info, side, picks, toks):
    info = jnp.concatenate([info, jnp.zeros((LANES - toks, INFO), jnp.float32)], axis=0)
    ids = info[:, :LANES].T[:picks]
    levels = info[:, LANES:].T[:picks]
    total = jnp.sum(levels, axis=0, keepdims=True)
    total = jnp.where(total == 0.0, 1.0, total)
    named, share = [], []
    for i in range(side):
        hit = ids == experts_ref[i].astype(jnp.float32)
        named.append(jnp.sum(jnp.where(hit, 1.0, 0.0), axis=0, keepdims=True))
        share.append(jnp.sum(jnp.where(hit, levels, 0.0), axis=0, keepdims=True) / total)
    per = toks // side
    a = lax.broadcasted_iota(jnp.int32, (LANES, LANES), 0)
    b = lax.broadcasted_iota(jnp.int32, (LANES, LANES), 1)
    earlier = jnp.where((a // per == b // per) & (a < b), 1.0, 0.0).astype(jnp.bfloat16)
    slot = jnp.dot(
        jnp.concatenate(named, axis=0).astype(jnp.bfloat16),
        earlier,
        preferred_element_type=jnp.float32,
    )
    own = (
        lax.broadcasted_iota(jnp.int32, (side, LANES), 1) // per
        == lax.broadcasted_iota(jnp.int32, (side, LANES), 0)
    )
    pieces, mixes = [], []
    for i in range(side):
        for s in range(CAP):
            here = jnp.where(slot[i : i + 1] == float(s), named[i], 0.0)
            pieces.append(jnp.where(own, here, 0.0))
            mixes.append(jnp.where(own, here * share[i], 0.0))
    select = jnp.concatenate(pieces, axis=0)[:, :toks].astype(jnp.bfloat16)
    count = select.shape[0]
    mix = jnp.concatenate(mixes + [jnp.zeros((-count % LANES, LANES), jnp.float32)], axis=0).T
    mix = mix[:toks, :count]
    high = mix.astype(jnp.bfloat16)
    rest = mix - high.astype(jnp.float32)
    mid = rest.astype(jnp.bfloat16)
    low = (rest - mid.astype(jnp.float32)).astype(jnp.bfloat16)
    return select, (high, mid, low)


def blocks(size, step):
    return [slice(n, n + step) for n in range(0, size, step)]


def spread(select, rows_ref, out_ref):
    for cols in blocks(out_ref.shape[1], 4 * LANES):
        out_ref[:, cols] = jnp.dot(
            select, rows_ref[:, cols], preferred_element_type=jnp.float32
        ).astype(jnp.bfloat16)


def route_kernel(experts_ref, rows_ref, *refs, side, picks):
    out_ref, mix_ref = refs[-2:]
    size = out_ref.shape[1]
    toks = rows_ref.shape[0]
    info = rows_ref[:, size:].astype(jnp.float32)
    select, mix = selection(experts_ref, info, side, picks, toks)
    for n, m in enumerate(mix):
        mix_ref[n * toks : (n + 1) * toks] = m
    spread(select, rows_ref, out_ref)


def expert_kernel(x_ref, *refs):
    weights, out_ref = refs[:6], refs[6]
    held, acc_ref, h_ref, sems = refs[7:13], refs[13], refs[14], refs[15]
    part = held[0].shape[1]
    width = x_ref.shape[1]
    pieces = blocks(width, width // STEPS)
    copies = []
    for k, rows in enumerate(pieces):
        copies.append([
            pltpu.make_async_copy(weights[n].at[0, rows], held[n].at[rows], sems.at[n, k])
            for n in range(4)
        ])
    for k, cols in enumerate(pieces):
        copies.append([
            pltpu.make_async_copy(weights[n].at[0, :, cols], held[n].at[:, cols], sems.at[n, k])
            for n in (4, 5)
        ])
    for group in copies:
        for copy in group:
            copy.start()
    for k, rows in enumerate(pieces):
        for copy in copies[k]:
            copy.wait()
        for n in range(4):
            cols = slice(n * part, (n + 1) * part)
            got = jnp.dot(x_ref[:, rows], held[n][rows], preferred_element_type=jnp.float32)
            acc_ref[:, cols] = acc_ref[:, cols] + got if k else got
    gate = acc_ref[:, : 2 * part]
    up = acc_ref[:, 2 * part :]
    h_ref[...] = (gate / (1.0 + jnp.exp(-gate)) * up).astype(jnp.bfloat16)
    for k, cols in enumerate(pieces):
        for copy in copies[STEPS + k]:
            copy.wait()
        out_ref[:, cols] = (
            jnp.dot(h_ref[:, :part], held[4][:, cols], preferred_element_type=jnp.float32)
            + jnp.dot(h_ref[:, part:], held[5][:, cols], preferred_element_type=jnp.float32)
        ).astype(jnp.bfloat16)


def mix_kernel(mix_ref, rows_ref, out_ref):
    toks = out_ref.shape[0]
    for cols in blocks(out_ref.shape[1], 4 * LANES):
        y = jnp.dot(mix_ref[...], rows_ref[:, cols], preferred_element_type=jnp.float32)
        out_ref[:, cols] = (y[:toks] + y[toks : 2 * toks] + y[2 * toks :]).astype(jnp.bfloat16)


def sum_kernel(rows_ref, out_ref):
    mine = out_ref.shape[0]
    total = rows_ref[:mine].astype(jnp.float32)
    for i in range(1, rows_ref.shape[0] // mine):
        total = total + rows_ref[i * mine : (i + 1) * mine].astype(jnp.float32)
    out_ref[...] = total.astype(jnp.bfloat16)


def local(tokens, expert_ids, route_levels, gate_proj, up_proj, down_proj):
    mine, width = tokens.shape
    picks = expert_ids.shape[1]
    side = math.isqrt(lax.axis_size("expert"))
    first, second = crossing_groups(side)
    core = lax.axis_index("sub")
    chip = lax.axis_index("expert")
    y, x = chip // side, chip % side
    i = jnp.arange(side, dtype=jnp.int32)
    experts = jnp.where(core == 0, (y * side + i) // 2, (i * side + x) // 2)
    toks = side * mine
    slots = toks * CAP
    part = gate_proj.shape[2]
    bf16, f32 = jnp.bfloat16, jnp.float32

    def crossed(block, groups):
        rows, cols = block.shape
        block = block.reshape(side, rows // side, cols)
        block = lax.all_to_all(block, GROUP, 0, 0, tiled=True, axis_index_groups=groups)
        return block.reshape(rows, cols)

    gate_peer, up_peer, down_peer = (
        lax.ppermute(w, "sub", [(0, 1), (1, 0)]) for w in (gate_proj, up_proj, down_proj)
    )

    rows = call(
        pack_kernel,
        [(tokens, PLAIN), (expert_ids, PLAIN), (route_levels, PLAIN)],
        [((toks, width + INFO), bf16, PLAIN)],
    )
    rows = crossed(rows, first)
    rows, mix = call(
        functools.partial(route_kernel, side=side, picks=picks),
        [(experts, S), (rows, V)] + [(w, A) for w in (gate_peer, up_peer, down_peer)],
        [((slots, width), bf16, V), ((3 * toks, slots), bf16, PLAIN)],
    )
    rows = crossed(rows, second)
    rows = call(
        expert_kernel,
        [(rows, V)]
        + [(w, A) for w in (gate_proj, gate_peer, up_proj, up_peer, down_proj, down_peer)],
        [((slots, width), bf16, V)],
        [V((width, part), bf16)] * 4
        + [V((part, width), bf16)] * 2
        + [V((slots, 4 * part), f32), V((slots, 2 * part), bf16)]
        + [pltpu.SemaphoreType.DMA((6, STEPS))],
        limit=36,
    )
    rows = crossed(rows, second)
    rows = call(mix_kernel, [(mix, PLAIN), (rows, V)], [((toks, width), bf16, V)])
    rows = crossed(rows, first)
    return call(sum_kernel, [(rows, V)], [((mine, width), bf16, PLAIN)])


def solution(mesh):
    return jax.shard_map(
        local,
        mesh=mesh,
        in_specs=(
            P(("replica", "expert", "sub"), None),
            P(("replica", "expert", "sub"), None),
            P(("replica", "expert", "sub"), None),
            P("expert", None, "sub"),
            P("expert", None, "sub"),
            P("expert", "sub", None),
        ),
        out_specs=P(("replica", "expert", "sub"), None),
        check_vma=False,
    )
```

```python
import functools
import math

import jax
import jax.numpy as jnp
from jax import lax
from jax.experimental import pallas as pl
from jax.experimental.pallas import tpu as pltpu
from jax.sharding import PartitionSpec as P


GROUP = ("expert", "sub")
LANES = 128
INFO = 2 * LANES
CAP = 3
STEPS = 4
MIB = 1 << 20


def device(side, y, x, c):
    return (y * side + x) * 2 + c


def first_groups(side):
    r = range(side)
    down = [[device(side, y, x, 0) for y in r] for x in r]
    over = [[device(side, y, x, 1) for x in r] for y in r]
    return down + over


def second_route(side, k):
    pairs = []
    for y in range(side):
        for x in range(side):
            over, down = (x + k) % side, (y + k) % side
            pairs.append((device(side, y, x, 0), device(side, y, over, 0)))
            pairs.append((device(side, y, x, 1), device(side, down, x, 1)))
    return pairs


def near_first(side):
    order = [0]
    for k in range(1, side // 2):
        order += [k, side - k]
    return order + [side // 2]


def held_in(x, space):
    return pltpu.with_memory_space_constraint(x, space)


V = pltpu.VMEM
S = pltpu.SMEM
A = pltpu.HBM
PLAIN = None


def call(kernel, ins, outs, scratch=(), limit=16):
    got = pl.pallas_call(
        kernel,
        in_specs=[pl.BlockSpec(memory_space=V if space is PLAIN else space) for _, space in ins],
        out_shape=[
            V(shape, dtype) if space is V else jax.ShapeDtypeStruct(shape, dtype)
            for shape, dtype, space in outs
        ],
        out_specs=[pl.BlockSpec(memory_space=V) for _ in outs],
        scratch_shapes=list(scratch),
        compiler_params=pltpu.CompilerParams(vmem_limit_bytes=limit * MIB),
    )(*[x if space is S else held_in(x, A if space is PLAIN else space) for x, space in ins])
    return got[0] if len(outs) == 1 else got


def pack_kernel(tokens_ref, ids_ref, levels_ref, out):
    mine, width = tokens_ref.shape
    picks = ids_ref.shape[1]
    rest = jnp.zeros((mine, LANES - picks), jnp.float32)
    info = [
        jnp.concatenate([r[...].astype(jnp.float32), rest], axis=1).astype(jnp.bfloat16)
        for r in (ids_ref, levels_ref)
    ]
    for i in range(out.shape[0] // mine):
        here = slice(i * mine, (i + 1) * mine)
        out[here, :width] = tokens_ref[...]
        out[here, width : width + LANES] = info[0]
        out[here, width + LANES :] = info[1]


def selection(experts_ref, info, side, picks, toks):
    info = jnp.concatenate([info, jnp.zeros((LANES - toks, INFO), jnp.float32)], axis=0)
    ids = info[:, :LANES].T[:picks]
    levels = info[:, LANES:].T[:picks]
    total = jnp.sum(levels, axis=0, keepdims=True)
    total = jnp.where(total == 0.0, 1.0, total)
    named, share = [], []
    for i in range(side):
        hit = ids == experts_ref[i].astype(jnp.float32)
        named.append(jnp.sum(jnp.where(hit, 1.0, 0.0), axis=0, keepdims=True))
        share.append(jnp.sum(jnp.where(hit, levels, 0.0), axis=0, keepdims=True) / total)
    per = toks // side
    a = lax.broadcasted_iota(jnp.int32, (LANES, LANES), 0)
    b = lax.broadcasted_iota(jnp.int32, (LANES, LANES), 1)
    earlier = jnp.where((a // per == b // per) & (a < b), 1.0, 0.0).astype(jnp.bfloat16)
    slot = jnp.dot(
        jnp.concatenate(named, axis=0).astype(jnp.bfloat16),
        earlier,
        preferred_element_type=jnp.float32,
    )
    own = (
        lax.broadcasted_iota(jnp.int32, (side, LANES), 1) // per
        == lax.broadcasted_iota(jnp.int32, (side, LANES), 0)
    )
    pieces, mixes = [], []
    for i in range(side):
        for s in range(CAP):
            here = jnp.where(slot[i : i + 1] == float(s), named[i], 0.0)
            pieces.append(jnp.where(own, here, 0.0))
            mixes.append(jnp.where(own, here * share[i], 0.0))
    select = jnp.concatenate(pieces, axis=0)[:, :toks].astype(jnp.bfloat16)
    count = select.shape[0]
    mix = jnp.concatenate(mixes + [jnp.zeros((-count % LANES, LANES), jnp.float32)], axis=0).T
    mix = mix[:toks, :count]
    high = mix.astype(jnp.bfloat16)
    rest = mix - high.astype(jnp.float32)
    mid = rest.astype(jnp.bfloat16)
    low = (rest - mid.astype(jnp.float32)).astype(jnp.bfloat16)
    return select, (high, mid, low)


def blocks(size, step):
    return [slice(n, n + step) for n in range(0, size, step)]


def put(outs, cols, got):
    each = outs[0].shape[0]
    for k, out in enumerate(outs):
        out[:, cols] = got[k * each : (k + 1) * each].astype(jnp.bfloat16)


def gathered(ref, rows):
    each = rows[0].shape[0]
    for k, r in enumerate(rows):
        ref[k * each : (k + 1) * each] = r[...]


def route_kernel(experts_ref, rows_ref, *refs, side, picks):
    outs, mix_ref = refs[-side - 1 : -1], refs[-1]
    width = outs[0].shape[1]
    toks = rows_ref.shape[0]
    info = rows_ref[:, width:].astype(jnp.float32)
    select, mix = selection(experts_ref, info, side, picks, toks)
    for n, m in enumerate(mix):
        mix_ref[n * toks : (n + 1) * toks] = m
    for cols in blocks(width, 4 * LANES):
        put(outs, cols, jnp.dot(select, rows_ref[:, cols], preferred_element_type=jnp.float32))


def expert_kernel(*refs, side):
    arrived, weights, outs = refs[:side], refs[side : side + 6], refs[side + 6 : 2 * side + 6]
    refs = refs[2 * side + 6 :]
    held, acc_ref, h_ref, x_ref, sems = refs[:6], refs[6], refs[7], refs[8], refs[9]
    part = held[0].shape[1]
    width = x_ref.shape[1]
    pieces = blocks(width, width // STEPS)
    copies = []
    for k, rows in enumerate(pieces):
        copies.append([
            pltpu.make_async_copy(weights[n].at[0, rows], held[n].at[rows], sems.at[n, k])
            for n in range(4)
        ])
    for k, cols in enumerate(pieces):
        copies.append([
            pltpu.make_async_copy(weights[n].at[0, :, cols], held[n].at[:, cols], sems.at[n, k])
            for n in (4, 5)
        ])
    for group in copies:
        for copy in group:
            copy.start()
    gathered(x_ref, arrived)
    for k, rows in enumerate(pieces):
        for copy in copies[k]:
            copy.wait()
        for n in range(4):
            cols = slice(n * part, (n + 1) * part)
            got = jnp.dot(x_ref[:, rows], held[n][rows], preferred_element_type=jnp.float32)
            acc_ref[:, cols] = acc_ref[:, cols] + got if k else got
    gate = acc_ref[:, : 2 * part]
    up = acc_ref[:, 2 * part :]
    h_ref[...] = (gate / (1.0 + jnp.exp(-gate)) * up).astype(jnp.bfloat16)
    for k, cols in enumerate(pieces):
        for copy in copies[STEPS + k]:
            copy.wait()
        put(
            outs,
            cols,
            jnp.dot(h_ref[:, :part], held[4][:, cols], preferred_element_type=jnp.float32)
            + jnp.dot(h_ref[:, part:], held[5][:, cols], preferred_element_type=jnp.float32),
        )


def mix_kernel(mix_ref, *refs):
    rows, out_ref, rows_ref = refs[:-2], refs[-2], refs[-1]
    toks = out_ref.shape[0]
    gathered(rows_ref, rows)
    for cols in blocks(out_ref.shape[1], 4 * LANES):
        y = jnp.dot(mix_ref[...], rows_ref[:, cols], preferred_element_type=jnp.float32)
        out_ref[:, cols] = (y[:toks] + y[toks : 2 * toks] + y[2 * toks :]).astype(jnp.bfloat16)


def sum_kernel(rows_ref, out_ref):
    mine = out_ref.shape[0]
    total = rows_ref[:mine].astype(jnp.float32)
    for i in range(1, rows_ref.shape[0] // mine):
        total = total + rows_ref[i * mine : (i + 1) * mine].astype(jnp.float32)
    out_ref[...] = total.astype(jnp.bfloat16)


def local(tokens, expert_ids, route_levels, gate_proj, up_proj, down_proj):
    mine, width = tokens.shape
    picks = expert_ids.shape[1]
    side = math.isqrt(lax.axis_size("expert"))
    order = near_first(side)
    core = lax.axis_index("sub")
    chip = lax.axis_index("expert")
    y, x = chip // side, chip % side
    k = jnp.array(order, dtype=jnp.int32)
    experts = jnp.where(
        core == 0, (y * side + (x + k) % side) // 2, ((y + k) % side * side + x) // 2
    )
    toks = side * mine
    slots = toks * CAP
    part = gate_proj.shape[2]
    bf16, f32 = jnp.bfloat16, jnp.float32

    each = slots // side

    def first_crossed(block):
        rows, cols = block.shape
        block = block.reshape(side, rows // side, cols)
        block = lax.all_to_all(block, GROUP, 0, 0, tiled=True, axis_index_groups=first_groups(side))
        return block.reshape(rows, cols)

    def second_crossed(rows, sign):
        moved = [rows[0]]
        for n in range(1, side):
            moved.append(lax.ppermute(rows[n], GROUP, second_route(side, sign * order[n])))
        return moved

    gate_peer, up_peer, down_peer = (
        lax.ppermute(w, "sub", [(0, 1), (1, 0)]) for w in (gate_proj, up_proj, down_proj)
    )

    rows = call(
        pack_kernel,
        [(tokens, PLAIN), (expert_ids, PLAIN), (route_levels, PLAIN)],
        [((toks, width + INFO), bf16, PLAIN)],
    )
    rows = first_crossed(rows)
    *rows, mix = call(
        functools.partial(route_kernel, side=side, picks=picks),
        [(experts, S), (rows, V)] + [(w, A) for w in (gate_peer, up_peer, down_peer)],
        [((each, width), bf16, V)] * side + [((3 * toks, slots), bf16, V)],
    )
    rows = second_crossed(rows, 1)
    rows = call(
        functools.partial(expert_kernel, side=side),
        [(r, V) for r in rows]
        + [(w, A) for w in (gate_proj, gate_peer, up_proj, up_peer, down_proj, down_peer)],
        [((each, width), bf16, V)] * side,
        [V((width, part), bf16)] * 4
        + [V((part, width), bf16)] * 2
        + [V((slots, 4 * part), f32), V((slots, 2 * part), bf16), V((slots, width), bf16)]
        + [pltpu.SemaphoreType.DMA((6, STEPS))],
        limit=36,
    )
    rows = second_crossed(rows, -1)
    rows = call(
        mix_kernel,
        [(mix, V)] + [(r, V) for r in rows],
        [((toks, width), bf16, V)],
        [V((slots, width), bf16)],
    )
    rows = first_crossed(rows)
    return call(sum_kernel, [(rows, V)], [((mine, width), bf16, PLAIN)])


def solution(mesh):
    return jax.shard_map(
        local,
        mesh=mesh,
        in_specs=(
            P(("replica", "expert", "sub"), None),
            P(("replica", "expert", "sub"), None),
            P(("replica", "expert", "sub"), None),
            P("expert", None, "sub"),
            P("expert", None, "sub"),
            P("expert", "sub", None),
        ),
        out_specs=P(("replica", "expert", "sub"), None),
        check_vma=False,
    )
```

```python
import functools
import math

import jax
import jax.numpy as jnp
from jax import lax
from jax.experimental import pallas as pl
from jax.experimental.pallas import tpu as pltpu
from jax.sharding import PartitionSpec as P


GROUP = ("expert", "sub")
LANES = 128
INFO = 2 * LANES
CAP = 3
MIB = 1 << 20


def device(side, y, x, c):
    return (y * side + x) * 2 + c


def route_pairs(side, k, stage):
    pairs = []
    for y in range(side):
        for x in range(side):
            over, down = (x + k) % side, (y + k) % side
            for c in (0, 1):
                far = (y, over) if c != stage else (down, x)
                pairs.append((device(side, y, x, c), device(side, *far, c)))
    return pairs


def near_first(side):
    order = [0]
    for k in range(1, side // 2):
        order += [k, side - k]
    return order + [side // 2]


def held_in(x, space):
    return pltpu.with_memory_space_constraint(x, space)


V = pltpu.VMEM
S = pltpu.SMEM
A = pltpu.HBM
PLAIN = None


def call(kernel, ins, outs, scratch=(), limit=16):
    got = pl.pallas_call(
        kernel,
        in_specs=[pl.BlockSpec(memory_space=V if space is PLAIN else space) for _, space in ins],
        out_shape=[
            V(shape, dtype) if space is V else jax.ShapeDtypeStruct(shape, dtype)
            for shape, dtype, space in outs
        ],
        out_specs=[pl.BlockSpec(memory_space=V) for _ in outs],
        scratch_shapes=list(scratch),
        compiler_params=pltpu.CompilerParams(vmem_limit_bytes=limit * MIB),
    )(*[x if space is S else held_in(x, A if space is PLAIN else space) for x, space in ins])
    return got[0] if len(outs) == 1 else got


def pack_kernel(tokens_ref, ids_ref, levels_ref, out):
    mine, width = tokens_ref.shape
    picks = ids_ref.shape[1]
    rest = jnp.zeros((mine, LANES - picks), jnp.float32)
    info = [
        jnp.concatenate([r[...].astype(jnp.float32), rest], axis=1).astype(jnp.bfloat16)
        for r in (ids_ref, levels_ref)
    ]
    out[:, :width] = tokens_ref[...]
    out[:, width : width + LANES] = info[0]
    out[:, width + LANES :] = info[1]


def selection(experts_ref, info, side, picks, toks):
    info = jnp.concatenate([info, jnp.zeros((LANES - toks, INFO), jnp.float32)], axis=0)
    ids = info[:, :LANES].T[:picks]
    levels = info[:, LANES:].T[:picks]
    total = jnp.sum(levels, axis=0, keepdims=True)
    total = jnp.where(total == 0.0, 1.0, total)
    named, share = [], []
    for i in range(side):
        hit = ids == experts_ref[i].astype(jnp.float32)
        named.append(jnp.sum(jnp.where(hit, 1.0, 0.0), axis=0, keepdims=True))
        share.append(jnp.sum(jnp.where(hit, levels, 0.0), axis=0, keepdims=True) / total)
    per = toks // side
    a = lax.broadcasted_iota(jnp.int32, (LANES, LANES), 0)
    b = lax.broadcasted_iota(jnp.int32, (LANES, LANES), 1)
    earlier = jnp.where((a // per == b // per) & (a < b), 1.0, 0.0).astype(jnp.bfloat16)
    slot = jnp.dot(
        jnp.concatenate(named, axis=0).astype(jnp.bfloat16),
        earlier,
        preferred_element_type=jnp.float32,
    )
    own = (
        lax.broadcasted_iota(jnp.int32, (side, LANES), 1) // per
        == lax.broadcasted_iota(jnp.int32, (side, LANES), 0)
    )
    pieces, mixes = [], []
    for i in range(side):
        for s in range(CAP):
            here = jnp.where(slot[i : i + 1] == float(s), named[i], 0.0)
            pieces.append(jnp.where(own, here, 0.0))
            mixes.append(jnp.where(own, here * share[i], 0.0))
    select = jnp.concatenate(pieces, axis=0)[:, :toks].astype(jnp.bfloat16)
    count = select.shape[0]
    mix = jnp.concatenate(mixes + [jnp.zeros((-count % LANES, LANES), jnp.float32)], axis=0).T
    mix = mix[:toks, :count]
    high = mix.astype(jnp.bfloat16)
    rest = mix - high.astype(jnp.float32)
    mid = rest.astype(jnp.bfloat16)
    low = (rest - mid.astype(jnp.float32)).astype(jnp.bfloat16)
    return select, (high, mid, low)


def blocks(size, step):
    return [slice(n, n + step) for n in range(0, size, step)]


def put(outs, cols, got):
    each = outs[0].shape[0]
    for k, out in enumerate(outs):
        out[:, cols] = got[k * each : (k + 1) * each].astype(jnp.bfloat16)


def gathered(ref, rows):
    each = rows[0].shape[0]
    for k, r in enumerate(rows):
        ref[k * each : (k + 1) * each] = r[...]


def route_kernel(experts_ref, *refs, side, picks):
    rows, outs, mix_ref, rows_ref = refs[:side], refs[side:-2], refs[-2], refs[-1]
    width = outs[0].shape[1]
    toks = rows_ref.shape[0]
    gathered(rows_ref, rows)
    info = rows_ref[:, width:].astype(jnp.float32)
    select, mix = selection(experts_ref, info, side, picks, toks)
    for n, m in enumerate(mix):
        mix_ref[n * toks : (n + 1) * toks] = m
    for cols in blocks(width, 4 * LANES):
        put(outs, cols, jnp.dot(select, rows_ref[:, cols], preferred_element_type=jnp.float32))


def load_kernel(*refs):
    count = len(refs) // 2
    sems = refs[-1]
    copies = [pltpu.make_async_copy(refs[n], refs[count + n], sems.at[n]) for n in range(count)]
    for copy in copies:
        copy.start()
    for copy in copies:
        copy.wait()


def expert_kernel(*refs, side):
    arrived, held, outs = refs[:side], refs[side : side + 6], refs[side + 6 : 2 * side + 6]
    acc_ref, h_ref, x_ref = refs[2 * side + 6 :]
    part = held[0].shape[2]
    gathered(x_ref, arrived)
    for n in range(4):
        cols = slice(n * part, (n + 1) * part)
        acc_ref[:, cols] = jnp.dot(x_ref[...], held[n][0], preferred_element_type=jnp.float32)
    gate = acc_ref[:, : 2 * part]
    up = acc_ref[:, 2 * part :]
    h_ref[...] = (gate / (1.0 + jnp.exp(-gate)) * up).astype(jnp.bfloat16)
    for cols in blocks(x_ref.shape[1], 4 * LANES):
        put(
            outs,
            cols,
            jnp.dot(h_ref[:, :part], held[4][0, :, cols], preferred_element_type=jnp.float32)
            + jnp.dot(h_ref[:, part:], held[5][0, :, cols], preferred_element_type=jnp.float32),
        )


def mix_kernel(mix_ref, *refs, side):
    rows, outs, rows_ref = refs[:side], refs[side:-1], refs[-1]
    toks = side * outs[0].shape[0]
    gathered(rows_ref, rows)
    for cols in blocks(rows_ref.shape[1], 4 * LANES):
        y = jnp.dot(mix_ref[...], rows_ref[:, cols], preferred_element_type=jnp.float32)
        put(outs, cols, y[:toks] + y[toks : 2 * toks] + y[2 * toks :])


def sum_kernel(*refs):
    total = refs[0][...].astype(jnp.float32)
    for r in refs[1:-1]:
        total = total + r[...].astype(jnp.float32)
    refs[-1][...] = total.astype(jnp.bfloat16)


def local(tokens, expert_ids, route_levels, gate_proj, up_proj, down_proj):
    mine, width = tokens.shape
    picks = expert_ids.shape[1]
    side = math.isqrt(lax.axis_size("expert"))
    order = near_first(side)
    core = lax.axis_index("sub")
    chip = lax.axis_index("expert")
    y, x = chip // side, chip % side
    k = jnp.array(order, dtype=jnp.int32)
    experts = jnp.where(
        core == 0, (y * side + (x + k) % side) // 2, ((y + k) % side * side + x) // 2
    )
    toks = side * mine
    slots = toks * CAP
    part = gate_proj.shape[2]
    bf16, f32 = jnp.bfloat16, jnp.float32

    each = slots // side


    def crossed(rows, stage, sign):
        moved = [rows[0]]
        for n in range(1, side):
            pairs = route_pairs(side, sign * order[n], stage)
            moved.append(lax.ppermute(rows[n], GROUP, pairs))
        return moved

    rows = call(
        pack_kernel,
        [(tokens, PLAIN), (expert_ids, PLAIN), (route_levels, PLAIN)],
        [((mine, width + INFO), bf16, V)],
    )
    rows = crossed([rows] * side, 0, 1)

    gate_peer, up_peer, down_peer = (
        lax.ppermute(w, "sub", [(0, 1), (1, 0)]) for w in (gate_proj, up_proj, down_proj)
    )

    *rows, mix = call(
        functools.partial(route_kernel, side=side, picks=picks),
        [(experts, S)] + [(r, V) for r in rows],
        [((each, width), bf16, V)] * side + [((3 * toks, slots), bf16, V)],
        [V((toks, width + INFO), bf16)],
    )
    rows = crossed(rows, 1, 1)
    weights = [gate_proj, gate_peer, up_proj, up_peer, down_proj, down_peer]
    weights = call(
        load_kernel,
        [(w, A) for w in weights],
        [(w.shape, bf16, V) for w in weights],
        [pltpu.SemaphoreType.DMA((len(weights),))],
    )
    rows = call(
        functools.partial(expert_kernel, side=side),
        [(r, V) for r in rows] + [(w, V) for w in weights],
        [((each, width), bf16, V)] * side,
        [V((slots, 4 * part), f32), V((slots, 2 * part), bf16), V((slots, width), bf16)],
    )
    rows = crossed(rows, 1, -1)
    rows = call(
        functools.partial(mix_kernel, side=side),
        [(mix, V)] + [(r, V) for r in rows],
        [((mine, width), bf16, V)] * side,
        [V((slots, width), bf16)],
    )
    rows = crossed(rows, 0, -1)
    return call(sum_kernel, [(r, V) for r in rows], [((mine, width), bf16, PLAIN)])


def solution(mesh):
    return jax.shard_map(
        local,
        mesh=mesh,
        in_specs=(
            P(("replica", "expert", "sub"), None),
            P(("replica", "expert", "sub"), None),
            P(("replica", "expert", "sub"), None),
            P("expert", None, "sub"),
            P("expert", None, "sub"),
            P("expert", "sub", None),
        ),
        out_specs=P(("replica", "expert", "sub"), None),
        check_vma=False,
    )
```

```python
import functools
import math

import jax
import jax.numpy as jnp
from jax import lax
from jax.experimental import pallas as pl
from jax.experimental.pallas import tpu as pltpu
from jax.sharding import PartitionSpec as P


GROUP = ("expert", "sub")
LANES = 128
INFO = 2 * LANES
CAP = 3
MIB = 1 << 20


def device(side, y, x, c):
    return (y * side + x) * 2 + c


def route_pairs(side, k, stage):
    pairs = []
    for y in range(side):
        for x in range(side):
            over, down = (x + k) % side, (y + k) % side
            for c in (0, 1):
                far = (y, over) if c != stage else (down, x)
                pairs.append((device(side, y, x, c), device(side, *far, c)))
    return pairs


def near_first(side):
    order = [0]
    for k in range(1, side // 2):
        order += [k, side - k]
    return order + [side // 2]


def held_in(x, space):
    return pltpu.with_memory_space_constraint(x, space)


V = pltpu.VMEM
S = pltpu.SMEM
A = pltpu.HBM
PLAIN = None


def call(kernel, ins, outs, scratch=(), limit=16):
    got = pl.pallas_call(
        kernel,
        in_specs=[pl.BlockSpec(memory_space=V if space is PLAIN else space) for _, space in ins],
        out_shape=[
            V(shape, dtype) if space is V else jax.ShapeDtypeStruct(shape, dtype)
            for shape, dtype, space in outs
        ],
        out_specs=[pl.BlockSpec(memory_space=V) for _ in outs],
        scratch_shapes=list(scratch),
        compiler_params=pltpu.CompilerParams(vmem_limit_bytes=limit * MIB),
    )(*[x if space is S else held_in(x, A if space is PLAIN else space) for x, space in ins])
    return got[0] if len(outs) == 1 else got


def pack_kernel(tokens_ref, ids_ref, levels_ref, out):
    mine, width = tokens_ref.shape
    picks = ids_ref.shape[1]
    rest = jnp.zeros((mine, LANES - picks), jnp.float32)
    info = [
        jnp.concatenate([r[...].astype(jnp.float32), rest], axis=1).astype(jnp.bfloat16)
        for r in (ids_ref, levels_ref)
    ]
    out[:, :width] = tokens_ref[...]
    out[:, width : width + LANES] = info[0]
    out[:, width + LANES :] = info[1]


def selection(experts_ref, info, side, picks, toks):
    info = jnp.concatenate([info, jnp.zeros((LANES - toks, INFO), jnp.float32)], axis=0)
    ids = info[:, :LANES].T[:picks]
    levels = info[:, LANES:].T[:picks]
    total = jnp.sum(levels, axis=0, keepdims=True)
    total = jnp.where(total == 0.0, 1.0, total)
    named, share = [], []
    for i in range(side):
        hit = ids == experts_ref[i].astype(jnp.float32)
        named.append(jnp.sum(jnp.where(hit, 1.0, 0.0), axis=0, keepdims=True))
        share.append(jnp.sum(jnp.where(hit, levels, 0.0), axis=0, keepdims=True) / total)
    per = toks // side
    a = lax.broadcasted_iota(jnp.int32, (LANES, LANES), 0)
    b = lax.broadcasted_iota(jnp.int32, (LANES, LANES), 1)
    earlier = jnp.where((a // per == b // per) & (a < b), 1.0, 0.0).astype(jnp.bfloat16)
    slot = jnp.dot(
        jnp.concatenate(named, axis=0).astype(jnp.bfloat16),
        earlier,
        preferred_element_type=jnp.float32,
    )
    own = (
        lax.broadcasted_iota(jnp.int32, (side, LANES), 1) // per
        == lax.broadcasted_iota(jnp.int32, (side, LANES), 0)
    )
    pieces, mixes = [], []
    for i in range(side):
        for s in range(CAP):
            here = jnp.where(slot[i : i + 1] == float(s), named[i], 0.0)
            pieces.append(jnp.where(own, here, 0.0))
            mixes.append(jnp.where(own, here * share[i], 0.0))
    select = jnp.concatenate(pieces, axis=0)[:, :toks].astype(jnp.bfloat16)
    count = select.shape[0]
    mix = jnp.concatenate(mixes + [jnp.zeros((-count % LANES, LANES), jnp.float32)], axis=0).T
    mix = mix[:toks, :count]
    high = mix.astype(jnp.bfloat16)
    rest = mix - high.astype(jnp.float32)
    mid = rest.astype(jnp.bfloat16)
    low = (rest - mid.astype(jnp.float32)).astype(jnp.bfloat16)
    return select, (high, mid, low)


def blocks(size, step):
    return [slice(n, n + step) for n in range(0, size, step)]


def put(outs, cols, got):
    each = outs[0].shape[0]
    for k, out in enumerate(outs):
        out[:, cols] = got[k * each : (k + 1) * each].astype(jnp.bfloat16)


def gathered(ref, rows):
    each = rows[0].shape[0]
    for k, r in enumerate(rows):
        ref[k * each : (k + 1) * each] = r[...]


def route_kernel(experts_ref, *refs, side, picks):
    rows, outs, mix_ref, rows_ref = refs[:side], refs[side:-2], refs[-2], refs[-1]
    width = outs[0].shape[1]
    toks = rows_ref.shape[0]
    gathered(rows_ref, rows)
    info = rows_ref[:, width:].astype(jnp.float32)
    select, mix = selection(experts_ref, info, side, picks, toks)
    for n, m in enumerate(mix):
        mix_ref[n * toks : (n + 1) * toks] = m
    for cols in blocks(width, 4 * LANES):
        put(outs, cols, jnp.dot(select, rows_ref[:, cols], preferred_element_type=jnp.float32))


def load_kernel(*refs):
    count = len(refs) // 2
    sems = refs[-1]
    copies = [pltpu.make_async_copy(refs[n], refs[count + n], sems.at[n]) for n in range(count)]
    for copy in copies:
        copy.start()
    for copy in copies:
        copy.wait()


def expert_kernel(*refs, count):
    arrived, held, outs = refs[:count], refs[count : count + 6], refs[count + 6 : 2 * count + 6]
    acc_ref, h_ref, x_ref = refs[2 * count + 6 :]
    part = held[0].shape[2]
    gathered(x_ref, arrived)
    for n in range(4):
        cols = slice(n * part, (n + 1) * part)
        acc_ref[:, cols] = jnp.dot(x_ref[...], held[n][0], preferred_element_type=jnp.float32)
    gate = acc_ref[:, : 2 * part]
    up = acc_ref[:, 2 * part :]
    h_ref[...] = (gate / (1.0 + jnp.exp(-gate)) * up).astype(jnp.bfloat16)
    for cols in blocks(x_ref.shape[1], 4 * LANES):
        put(
            outs,
            cols,
            jnp.dot(h_ref[:, :part], held[4][0, :, cols], preferred_element_type=jnp.float32)
            + jnp.dot(h_ref[:, part:], held[5][0, :, cols], preferred_element_type=jnp.float32),
        )


def mix_kernel(mix_ref, *refs, side):
    rows, outs, rows_ref = refs[:side], refs[side:-1], refs[-1]
    toks = side * outs[0].shape[0]
    gathered(rows_ref, rows)
    for cols in blocks(rows_ref.shape[1], 4 * LANES):
        y = jnp.dot(mix_ref[...], rows_ref[:, cols], preferred_element_type=jnp.float32)
        put(outs, cols, y[:toks] + y[toks : 2 * toks] + y[2 * toks :])


def sum_kernel(*refs):
    total = refs[0][...].astype(jnp.float32)
    for r in refs[1:-1]:
        total = total + r[...].astype(jnp.float32)
    refs[-1][...] = total.astype(jnp.bfloat16)


def local(tokens, expert_ids, route_levels, gate_proj, up_proj, down_proj):
    mine, width = tokens.shape
    picks = expert_ids.shape[1]
    side = math.isqrt(lax.axis_size("expert"))
    order = near_first(side)
    core = lax.axis_index("sub")
    chip = lax.axis_index("expert")
    y, x = chip // side, chip % side
    k = jnp.array(order, dtype=jnp.int32)
    experts = jnp.where(
        core == 0, (y * side + (x + k) % side) // 2, ((y + k) % side * side + x) // 2
    )
    toks = side * mine
    slots = toks * CAP
    part = gate_proj.shape[2]
    bf16, f32 = jnp.bfloat16, jnp.float32

    each = slots // side


    def crossed(rows, n, stage, sign):
        if not n:
            return rows
        return lax.ppermute(rows, GROUP, route_pairs(side, sign * order[n], stage))

    rows = call(
        pack_kernel,
        [(tokens, PLAIN), (expert_ids, PLAIN), (route_levels, PLAIN)],
        [((mine, width + INFO), bf16, V)],
    )
    rows = [crossed(rows, n, 0, 1) for n in range(side)]

    gate_peer, up_peer, down_peer = (
        lax.ppermute(w, "sub", [(0, 1), (1, 0)]) for w in (gate_proj, up_proj, down_proj)
    )

    *rows, mix = call(
        functools.partial(route_kernel, side=side, picks=picks),
        [(experts, S)] + [(r, V) for r in rows],
        [((each, width), bf16, V)] * side + [((3 * toks, slots), bf16, V)],
        [V((toks, width + INFO), bf16)],
    )
    rows = [crossed(r, n, 1, 1) for n, r in enumerate(rows)]
    gate, up, down = call(
        load_kernel,
        [(w, A) for w in (gate_proj, up_proj, down_proj)],
        [(w.shape, bf16, V) for w in (gate_proj, up_proj, down_proj)],
        [pltpu.SemaphoreType.DMA((3,))],
    )

    near = side // 2 + 1
    for blocks_here in (range(near, side), range(near)):
        count = len(blocks_here)
        done = call(
            functools.partial(expert_kernel, count=count),
            [(rows[n], V) for n in blocks_here]
            + [(w, V) for w in (gate, gate_peer, up, up_peer, down, down_peer)],
            [((each, width), bf16, V)] * count,
            [
                V((count * each, 4 * part), f32),
                V((count * each, 2 * part), bf16),
                V((count * each, width), bf16),
            ],
        )
        for n, block in zip(blocks_here, done):
            rows[n] = crossed(block, n, 1, -1)
    rows = call(
        functools.partial(mix_kernel, side=side),
        [(mix, V)] + [(r, V) for r in rows],
        [((mine, width), bf16, V)] * side,
        [V((slots, width), bf16)],
    )
    rows = [crossed(r, n, 0, -1) for n, r in enumerate(rows)]
    return call(sum_kernel, [(r, V) for r in rows], [((mine, width), bf16, PLAIN)])


def solution(mesh):
    return jax.shard_map(
        local,
        mesh=mesh,
        in_specs=(
            P(("replica", "expert", "sub"), None),
            P(("replica", "expert", "sub"), None),
            P(("replica", "expert", "sub"), None),
            P("expert", None, "sub"),
            P("expert", None, "sub"),
            P("expert", "sub", None),
        ),
        out_specs=P(("replica", "expert", "sub"), None),
        check_vma=False,
    )
```

```python
import functools
import math

import jax
import jax.numpy as jnp
from jax import lax
from jax.experimental import pallas as pl
from jax.experimental.pallas import tpu as pltpu
from jax.sharding import PartitionSpec as P


GROUP = ("expert", "sub")
LANES = 128
INFO = 2 * LANES
CAP = 3
MIB = 1 << 20


def device(side, y, x, c):
    return (y * side + x) * 2 + c


def route_pairs(side, k, stage):
    pairs = []
    for y in range(side):
        for x in range(side):
            over, down = (x + k) % side, (y + k) % side
            for c in (0, 1):
                far = (y, over) if c != stage else (down, x)
                pairs.append((device(side, y, x, c), device(side, *far, c)))
    return pairs


def near_first(side):
    order = [0]
    for k in range(1, side // 2):
        order += [k, side - k]
    return order + [side // 2]


def held_in(x, space):
    return pltpu.with_memory_space_constraint(x, space)


V = pltpu.VMEM
S = pltpu.SMEM
A = pltpu.HBM
PLAIN = None


def call(kernel, ins, outs, scratch=(), limit=16):
    got = pl.pallas_call(
        kernel,
        in_specs=[pl.BlockSpec(memory_space=V if space is PLAIN else space) for _, space in ins],
        out_shape=[
            V(shape, dtype) if space is V else jax.ShapeDtypeStruct(shape, dtype)
            for shape, dtype, space in outs
        ],
        out_specs=[pl.BlockSpec(memory_space=V) for _ in outs],
        scratch_shapes=list(scratch),
        compiler_params=pltpu.CompilerParams(vmem_limit_bytes=limit * MIB),
    )(*[x if space is S else held_in(x, A if space is PLAIN else space) for x, space in ins])
    return got[0] if len(outs) == 1 else got


def pack_kernel(tokens_ref, ids_ref, levels_ref, out):
    mine, width = tokens_ref.shape
    picks = ids_ref.shape[1]
    rest = jnp.zeros((mine, LANES - picks), jnp.float32)
    info = [
        jnp.concatenate([r[...].astype(jnp.float32), rest], axis=1).astype(jnp.bfloat16)
        for r in (ids_ref, levels_ref)
    ]
    out[:, :width] = tokens_ref[...]
    out[:, width : width + LANES] = info[0]
    out[:, width + LANES :] = info[1]


def selection(experts_ref, info, side, picks, toks):
    info = jnp.concatenate([info, jnp.zeros((LANES - toks, INFO), jnp.float32)], axis=0)
    ids = info[:, :LANES].T[:picks]
    levels = info[:, LANES:].T[:picks]
    total = jnp.sum(levels, axis=0, keepdims=True)
    total = jnp.where(total == 0.0, 1.0, total)
    named, share = [], []
    for i in range(side):
        hit = ids == experts_ref[i].astype(jnp.float32)
        named.append(jnp.sum(jnp.where(hit, 1.0, 0.0), axis=0, keepdims=True))
        share.append(jnp.sum(jnp.where(hit, levels, 0.0), axis=0, keepdims=True) / total)
    per = toks // side
    a = lax.broadcasted_iota(jnp.int32, (LANES, LANES), 0)
    b = lax.broadcasted_iota(jnp.int32, (LANES, LANES), 1)
    earlier = jnp.where((a // per == b // per) & (a < b), 1.0, 0.0).astype(jnp.bfloat16)
    slot = jnp.dot(
        jnp.concatenate(named, axis=0).astype(jnp.bfloat16),
        earlier,
        preferred_element_type=jnp.float32,
    )
    own = (
        lax.broadcasted_iota(jnp.int32, (side, LANES), 1) // per
        == lax.broadcasted_iota(jnp.int32, (side, LANES), 0)
    )
    pieces, mixes = [], []
    for i in range(side):
        for s in range(CAP):
            here = jnp.where(slot[i : i + 1] == float(s), named[i], 0.0)
            pieces.append(jnp.where(own, here, 0.0))
            mixes.append(jnp.where(own, here * share[i], 0.0))
    select = jnp.concatenate(pieces, axis=0)[:, :toks].astype(jnp.bfloat16)
    count = select.shape[0]
    mix = jnp.concatenate(mixes + [jnp.zeros((-count % LANES, LANES), jnp.float32)], axis=0).T
    mix = mix[:toks, :count]
    high = mix.astype(jnp.bfloat16)
    rest = mix - high.astype(jnp.float32)
    mid = rest.astype(jnp.bfloat16)
    low = (rest - mid.astype(jnp.float32)).astype(jnp.bfloat16)
    return select, (high, mid, low)


def blocks(size, step):
    return [slice(n, n + step) for n in range(0, size, step)]


def put(outs, cols, got):
    each = outs[0].shape[0]
    for k, out in enumerate(outs):
        out[:, cols] = got[k * each : (k + 1) * each].astype(jnp.bfloat16)


def gathered(ref, rows):
    each = rows[0].shape[0]
    for k, r in enumerate(rows):
        ref[k * each : (k + 1) * each] = r[...]


def route_kernel(experts_ref, *refs, side, picks):
    rows, outs, mix_ref, rows_ref = refs[:side], refs[side:-2], refs[-2], refs[-1]
    width = outs[0].shape[1]
    toks = rows_ref.shape[0]
    gathered(rows_ref, rows)
    info = rows_ref[:, width:].astype(jnp.float32)
    select, mix = selection(experts_ref, info, side, picks, toks)
    for n, m in enumerate(mix):
        mix_ref[n * toks : (n + 1) * toks] = m
    for cols in blocks(width, 4 * LANES):
        put(outs, cols, jnp.dot(select, rows_ref[:, cols], preferred_element_type=jnp.float32))


def load_kernel(*refs):
    count = len(refs) // 2
    sems = refs[-1]
    copies = [pltpu.make_async_copy(refs[n], refs[count + n], sems.at[n]) for n in range(count)]
    for copy in copies:
        copy.start()
    for copy in copies:
        copy.wait()


def expert_kernel(*refs, count):
    arrived, held, outs = refs[:count], refs[count : count + 6], refs[count + 6 : 2 * count + 6]
    acc_ref, h_ref, x_ref = refs[2 * count + 6 :]
    part = held[0].shape[2]
    gathered(x_ref, arrived)
    for n in range(4):
        cols = slice(n * part, (n + 1) * part)
        acc_ref[:, cols] = jnp.dot(x_ref[...], held[n][0], preferred_element_type=jnp.float32)
    gate = acc_ref[:, : 2 * part]
    up = acc_ref[:, 2 * part :]
    h_ref[...] = (gate / (1.0 + jnp.exp(-gate)) * up).astype(jnp.bfloat16)
    for cols in blocks(x_ref.shape[1], 4 * LANES):
        put(
            outs,
            cols,
            jnp.dot(h_ref[:, :part], held[4][0, :, cols], preferred_element_type=jnp.float32)
            + jnp.dot(h_ref[:, part:], held[5][0, :, cols], preferred_element_type=jnp.float32),
        )


def mix_kernel(mix_ref, *refs, side):
    rows, outs, rows_ref = refs[:side], refs[side:-1], refs[-1]
    toks = side * outs[0].shape[0]
    gathered(rows_ref, rows)
    for cols in blocks(rows_ref.shape[1], 4 * LANES):
        y = jnp.dot(mix_ref[...], rows_ref[:, cols], preferred_element_type=jnp.float32)
        put(outs, cols, y[:toks] + y[toks : 2 * toks] + y[2 * toks :])


def sum_kernel(*refs):
    total = refs[0][...].astype(jnp.float32)
    for r in refs[1:-1]:
        total = total + r[...].astype(jnp.float32)
    refs[-1][...] = total.astype(jnp.bfloat16)


def local(tokens, expert_ids, route_levels, gate_proj, up_proj, down_proj):
    mine, width = tokens.shape
    picks = expert_ids.shape[1]
    side = math.isqrt(lax.axis_size("expert"))
    order = near_first(side)
    core = lax.axis_index("sub")
    chip = lax.axis_index("expert")
    y, x = chip // side, chip % side
    k = jnp.array(order, dtype=jnp.int32)
    experts = jnp.where(
        core == 0, (y * side + (x + k) % side) // 2, ((y + k) % side * side + x) // 2
    )
    toks = side * mine
    slots = toks * CAP
    part = gate_proj.shape[2]
    bf16, f32 = jnp.bfloat16, jnp.float32

    each = slots // side


    def crossed(rows, n, stage, sign):
        if not n:
            return rows
        return lax.ppermute(rows, GROUP, route_pairs(side, sign * order[n], stage))

    rows = call(
        pack_kernel,
        [(tokens, PLAIN), (expert_ids, PLAIN), (route_levels, PLAIN)],
        [((mine, width + INFO), bf16, V)],
    )
    rows = [crossed(rows, n, 0, 1) for n in range(side)]

    gate_peer, up_peer, down_peer = (
        lax.ppermute(w, "sub", [(0, 1), (1, 0)]) for w in (gate_proj, up_proj, down_proj)
    )

    *rows, mix = call(
        functools.partial(route_kernel, side=side, picks=picks),
        [(experts, S)] + [(r, V) for r in rows],
        [((each, width), bf16, V)] * side + [((3 * toks, slots), bf16, V)],
        [V((toks, width + INFO), bf16)],
    )
    rows = [crossed(r, n, 1, 1) for n, r in enumerate(rows)]
    weights = [gate_proj, gate_peer, up_proj, up_peer, down_proj, down_peer]
    weights = call(
        load_kernel,
        [(w, A) for w in weights],
        [(w.shape, bf16, V) for w in weights],
        [pltpu.SemaphoreType.DMA((len(weights),))],
    )

    near = side // 2 + 1
    for blocks_here in (range(near, side), range(near)):
        count = len(blocks_here)
        done = call(
            functools.partial(expert_kernel, count=count),
            [(rows[n], V) for n in blocks_here]
            + [(w, V) for w in weights],
            [((each, width), bf16, V)] * count,
            [
                V((count * each, 4 * part), f32),
                V((count * each, 2 * part), bf16),
                V((count * each, width), bf16),
            ],
        )
        for n, block in zip(blocks_here, done):
            rows[n] = crossed(block, n, 1, -1)
    rows = call(
        functools.partial(mix_kernel, side=side),
        [(mix, V)] + [(r, V) for r in rows],
        [((mine, width), bf16, V)] * side,
        [V((slots, width), bf16)],
    )
    rows = [crossed(r, n, 0, -1) for n, r in enumerate(rows)]
    return call(sum_kernel, [(r, V) for r in rows], [((mine, width), bf16, PLAIN)])


def solution(mesh):
    return jax.shard_map(
        local,
        mesh=mesh,
        in_specs=(
            P(("replica", "expert", "sub"), None),
            P(("replica", "expert", "sub"), None),
            P(("replica", "expert", "sub"), None),
            P("expert", None, "sub"),
            P("expert", None, "sub"),
            P("expert", "sub", None),
        ),
        out_specs=P(("replica", "expert", "sub"), None),
        check_vma=False,
    )
```
